128 devices in a mesh: row: 8 (over z, core), col: 16 (over y, x).
Axes of the slice: x: 4, y: 4, z: 4, core: 2. Of those that a mesh axis runs over, the one named last changes fastest.
Arguments:
- ainv_anc: bfloat16 [24576, 24576], P('row', 'col'), may hold values from -6 to 6
- l_panel: bfloat16 [1536, 24576], P('col', 'row'), may hold values from -0.078125 to 0.078125
- diag_inv: float32 [1536, 768], P('col', 'row'), may hold values from -6 to 6
- struct_mask: int32 [2, 192], replicated, may hold values 0 or 1
- pieces: float32 [24576, 32, 128], P(('row', 'col')), may hold values from -6 to 6
- tile_owner: int32 [24576, 1], P(('row', 'col')), may hold values from 0 to 127; in each aligned block of 192 rows (0 to 191, 192 to 383, ...) at most 3 rows name the same one
Outputs:
- ainv_upper: bfloat16 [1536, 24576], P('col', 'row')
- ainv_diag: float32 [1536, 768], P('col', 'row')
- moved: float32 [49152, 32, 128], P(('row', 'col'))
The draws below stay inside these ranges and needn't reach their ends.
Inputs may be any that keep to these rules, and one draw needn't show every extreme that they name: `tile_owner`: among the 192 pieces of one device no owner is named more than 3 times, a bound that some block reaches.
All inputs are finite; a program needn't handle non-finite values.
Results may differ from the reference program's by a relative error of at most 0.015.
Values may be sent and summed in bfloat16 or wider, within the bound.
No kernel may reach another device: no remote copies, remote signals or barrier semaphores. Data moves between devices by JAX's collectives and lax.ppermute only.
A program may use at most 128 MiB of HBM per device.

```python
import math
import jax
import jax.numpy as jnp
import numpy as np
from jax import lax

W = 768
NS = 2
AB = 128
SLOT = 3
TR = 32
TC = 128
ORDER = 24576
PANEL = 1536
NBLK = 192
TPD = 192
PIECES = 24576
N_ROW = 8
N_COL = 16
DEVICES = 128


def touch_ends(values, key, least, top_value):
    dims = values.shape
    index_at = [jax.random.randint(jax.random.fold_in(key, axis), (), 0, dims[axis]) for axis in range(len(dims))]
    values = values.at[tuple(index_at)].set(least)
    longest = dims.index(max(dims))
    index_at[longest] = (index_at[longest] + 1) % dims[longest]
    return values.at[tuple(index_at)].set(top_value)


def raised(values, own_key, source, target, parts, factor):
    def block_of(position):
        return (jnp.arange(values.shape[position]) // (values.shape[position] // parts)).reshape((-1,) + (1,) * (values.ndim - 1 - position))

    one_side = jax.random.permutation(own_key, parts)[block_of(target)]
    second = (block_of(target) + parts // 2) % parts
    return jnp.where((block_of(source) == one_side) | (block_of(source) == second), factor * values, values)


def shard_levels(key, extent, cuts, smallest, top_value):
    def one(position, parts):
        heights = jax.random.uniform(jax.random.fold_in(jax.random.fold_in(key, 6), position), (parts,), jnp.float32, smallest / len(cuts), top_value / len(cuts))
        return jnp.repeat(jnp.exp(heights), extent[position] // parts).reshape((-1,) + (1,) * (len(extent) - position - 1))

    loudness = one(*cuts[0])
    for cut in cuts[1:]:
        loudness = loudness * one(*cut)
    return loudness


def shared_out(key, own, number, rows, count, top, bound, skew):
    sequence = jax.random.permutation(key, count)
    crowded, common = load_shares(count, rows * top, bound, skew, True), load_shares(count, rows * top, bound, skew, False)
    places = jnp.arange(count)

    def named(tallies, offset_by):
        used = int((tallies > 0).sum())
        fixed = max(1, used // 4)
        passed = fixed + (places - fixed + offset_by * (used - fixed)) % max(1, count - fixed)
        return jnp.zeros((count,), jnp.int32).at[sequence[jnp.where(places < fixed, places, passed)]].set(jnp.asarray(tallies, jnp.int32))

    tallies = jnp.where(number % 4 == 0, named(crowded, number // 4), named(common, number - number // 4 - 1))
    mixed = jax.random.permutation(jax.random.fold_in(own, 3), count)
    donor, receiver = mixed[0:count // 2 * 2:2], mixed[1:count // 2 * 2:2]
    slack = jnp.minimum(tallies[donor] - 1, bound - tallies[receiver]) // 2
    slack = jnp.where((donor == sequence[0]) | (receiver == sequence[0]) | (tallies[receiver] == 0), 0, jnp.maximum(slack, 0))
    passed = jax.random.randint(jax.random.fold_in(own, 4), (count // 2,), 0, 1 << 20) % (slack + 1)
    tallies = tallies.at[donor].add(-passed).at[receiver].add(passed)
    members = jnp.searchsorted(jnp.cumsum(tallies), jnp.arange(rows * top), side="right").astype(jnp.int32)
    listing = members.reshape(top, rows).T
    listing = listing[jax.random.permutation(jax.random.fold_in(own, 1), rows)]
    offset_by = jax.random.randint(jax.random.fold_in(own, 2), (rows, 1), 0, top)
    return jnp.take_along_axis(listing, (jnp.arange(top)[None, :] + offset_by) % top, axis=1)


def load_shares(count, total, reach, lean, full):
    loads = [(1 << 20) // math.isqrt(grade ** lean) + 1 for grade in range(1, count + 1)]
    largest = reach if full else min(reach, max(-(-total // count), total * loads[0] // sum(loads)))
    least = 1 if total - largest >= count - 1 else 0
    holding, spare = [largest] + [least] * (count - 1), total - largest - least * (count - 1)
    while spare > 0:
        free = [i for i in range(1, count) if holding[i] < largest] or [i for i in range(1, count) if holding[i] < reach]
        pool, remaining = sum([loads[i] for i in free]), spare
        for i in free:
            more = min(reach - holding[i], max(1, remaining * loads[i] // pool), spare)
            holding[i] = holding[i] + more
            spare = spare - more
    return np.array(holding)


def noise(key, shape, deviation, most, cuts=(), held_as=jnp.bfloat16):
    result = jax.random.normal(key, shape, jnp.float32) * deviation
    if len(cuts) > 0:
        result = shard_levels(key, shape, cuts, -0.22, 0.18) * result
    return jnp.clip(result, min=-most, max=most).astype(held_as)


def noise_with(rng, extent, width, bound, cuts, heavy, held_as=jnp.bfloat16):
    values = width * jax.random.normal(rng, extent, jnp.float32)
    if cuts:
        values = values * shard_levels(rng, extent, cuts, -0.22, 0.18)
    return jnp.clip(raised(values, jax.random.fold_in(rng, 3), *heavy), -bound, bound).astype(held_as)


def setup_inputs(seed: int = 0) -> dict:
    seeds = jax.random.split(jax.random.key(seed), 7)
    ainv_anc = noise(seeds[0], (ORDER, ORDER), 1.0, 6.0, ((0, 8), (1, 16)))
    l_panel = noise_with(seeds[1], (PANEL, ORDER), (ORDER // 2) ** -0.5, 0.078125, ((0, 16), (1, 8)), (1, 0, 16, 2.0))
    diag_inv = noise(seeds[2], (PANEL, W), 1.0, 6.0, ((0, 16), (1, 8)), jnp.float32)
    struct_mask = touch_ends((jax.random.randint(seeds[3], (NS, NBLK), 0, 2) < 1).astype(jnp.int32), jax.random.fold_in(seeds[3], 1), 0, 1)
    pieces = noise(seeds[4], (PIECES, TR, TC), 1.0, 6.0, ((0, 128),), jnp.float32)
    tile_owner_keys = jax.random.split(jax.random.fold_in(seeds[5], 1), PIECES // TPD)
    tile_owner_turns = jax.random.permutation(jax.random.fold_in(seeds[5], 3), PIECES // TPD)
    tile_owner = jax.vmap(lambda own, number: shared_out(jax.random.fold_in(seeds[5], 2), own, number, TPD, DEVICES, 1, SLOT, 2))(tile_owner_keys, tile_owner_turns).reshape((PIECES, 1))
    return dict(ainv_anc=ainv_anc, l_panel=l_panel, diag_inv=diag_inv, struct_mask=struct_mask, pieces=pieces, tile_owner=tile_owner)


def mask_panel(l_panel, struct_mask):
    blocks = jnp.repeat(struct_mask, AB, axis=1)
    keep = blocks[:, None, :] > 0
    shaped = l_panel.reshape(NS, W, ORDER)
    masked = jnp.where(keep, shaped, jnp.zeros_like(shaped))
    return masked.reshape(NS * W, ORDER), keep


def reference(ainv_anc, l_panel, diag_inv, struct_mask, pieces, tile_owner):
    masked_panel, keep = mask_panel(l_panel, struct_mask)
    group_width = ORDER // N_COL

    def add_group(index, total):
        begin = (index * group_width).astype(jnp.int32)
        panel_cols = lax.dynamic_slice_in_dim(masked_panel, begin, group_width, 1)
        inverse_cols = lax.dynamic_slice_in_dim(ainv_anc, begin, group_width, 1)
        term = lax.dot_general(panel_cols, inverse_cols, (((1,), (1,)), ((), ())), preferred_element_type=jnp.float32)
        rounded = lax.optimization_barrier(term.astype(jnp.bfloat16))
        return total + rounded.astype(jnp.float32)

    product = lax.fori_loop(0, N_COL, add_group, jnp.zeros((NS * W, ORDER), jnp.float32))
    shaped = product.reshape(NS, W, ORDER)
    upper_rows = jnp.where(keep, -shaped, jnp.zeros_like(shaped)).reshape(NS * W, ORDER).astype(jnp.bfloat16)
    diag_blocks = []
    for supernode in range(NS):
        upper_part = upper_rows[supernode * W:(supernode + 1) * W]
        panel_part = masked_panel[supernode * W:(supernode + 1) * W]
        diag_blocks.append(lax.dot_general(upper_part, panel_part, (((1,), (1,)), ((), ())), preferred_element_type=jnp.float32))
    ainv_diag = diag_inv - jnp.concatenate(diag_blocks, axis=0)
    devices_all = N_ROW * N_COL
    owners = tile_owner[:, 0].reshape(devices_all, TPD)
    onehot = (owners[:, :, None] == jnp.arange(devices_all, dtype=jnp.int32)[None, None, :]).astype(jnp.int32)
    earlier = jnp.cumsum(onehot, axis=1) - onehot
    rank_in_dest = jnp.sum(earlier * onehot, axis=2)
    source = jnp.arange(devices_all, dtype=jnp.int32)[:, None]
    slot_index = ((owners * devices_all + source) * SLOT + rank_in_dest).reshape(-1).astype(jnp.int32)
    moved = jnp.zeros((devices_all * devices_all * SLOT, TR, TC), jnp.float32).at[slot_index].set(pieces)
    return upper_rows, ainv_diag, moved
```

```python
import jax
import jax.numpy as jnp
from jax import lax
from jax.experimental import pallas as pl
from jax.experimental.pallas import tpu as pltpu
from jax.sharding import PartitionSpec as P

W = 768
AB = 128
SLOT = 3
BOTH = ("row", "col")


def device_at(z, k, y, x):
    return ((z % 4) * 2 + k) * 16 + (y % 4) * 4 + x % 4


def move(value, to):
    pairs = [
        (device_at(z, k, y, x), device_at(*to(z, k, y, x)))
        for z in range(4)
        for k in range(2)
        for y in range(4)
        for x in range(4)
    ]
    return lax.ppermute(value, BOTH, pairs)


def along(axis, step):
    def to(z, k, y, x):
        at = dict(z=z, y=y, x=x)
        at[axis] += step
        return at["z"], k, at["y"], at["x"]

    return to


def other_core(z, k, y, x):
    return z, 1 - k, y, x


def pair_y(z, k, y, x):
    return z, k, y ^ 1, x


def to_group(p):
    def to(z, k, y, x):
        col = 2 * (2 * z + k) + (x % 2 ^ p)
        return y, x // 2, col // 4, col % 4

    return to


def pack_kernel(owner, pieces, packed, counts):
    packed[...] = jnp.zeros(packed.shape, packed.dtype)

    def clear(i, carry):
        counts[i] = 0
        return carry

    lax.fori_loop(0, counts.shape[0], clear, 0)

    def place(p, carry):
        to = owner[p]
        rank = counts[to]
        counts[to] = rank + 1
        packed[to * SLOT + rank] = pieces[p].astype(packed.dtype)
        return carry

    lax.fori_loop(0, pieces.shape[0], place, 0)


def pack(owners, pieces, devices):
    count, rows, cols = pieces.shape
    return pl.pallas_call(
        pack_kernel,
        out_shape=jax.ShapeDtypeStruct((devices * SLOT, rows, cols), jnp.bfloat16),
        grid_spec=pltpu.PrefetchScalarGridSpec(
            num_scalar_prefetch=1,
            grid=(1,),
            in_specs=[pl.BlockSpec((count, rows, cols), lambda i, owner: (0, 0, 0))],
            out_specs=pl.BlockSpec((devices * SLOT, rows, cols), lambda i, owner: (0, 0, 0)),
            scratch_shapes=[pltpu.SMEM((devices,), jnp.int32)],
        ),
        name="pack",
    )(owners, pieces)


def times(rows, ainv):
    flat = rows.reshape(-1, rows.shape[-1])
    out = lax.dot_general(
        flat, ainv, (((1,), (1,)), ((), ())), preferred_element_type=jnp.float32
    ).astype(jnp.bfloat16)
    return lax.optimization_barrier(out.reshape(*rows.shape[:-1], ainv.shape[0]))


def f32(value):
    return value.astype(jnp.float32)


def ring_sum(axis, far, ahead, behind, own):
    half = own.shape[-1] // 2
    up, down = along(axis, 1), along(axis, -1)
    far_up = move(far[..., :half], up)
    far_down = move(far[..., half:], down)
    only_up = move(ahead[..., half:], up)
    only_down = move(behind[..., :half], down)
    sum_up = move((f32(ahead[..., :half]) + f32(far_up)).astype(jnp.bfloat16), up)
    sum_down = move((f32(behind[..., half:]) + f32(far_down)).astype(jnp.bfloat16), down)
    left = f32(own[..., :half]) + f32(sum_up) + f32(only_down)
    right = f32(own[..., half:]) + f32(sum_down) + f32(only_up)
    return left, right


def direct_sum(axis, far, ahead, behind, own):
    far = move(far, along(axis, 2))
    ahead = move(ahead, along(axis, 1))
    behind = move(behind, along(axis, -1))
    return own + f32(far) + f32(ahead) + f32(behind)


def at_first(value, index):
    return lax.dynamic_index_in_dim(value, index, 0, keepdims=False)


def rolled(value, amount):
    value = jnp.where(amount % 2 == 1, jnp.roll(value, 1, axis=0), value)
    return jnp.where(amount // 2 % 2 == 1, jnp.roll(value, 2, axis=0), value)


def gathered_rows(lm):
    half = lm.shape[1] // 2
    up, down = along("x", 1), along("x", -1)
    out = []
    partner = move(lm, pair_y)
    for own in (lm, partner):
        ahead = move(own, up)
        behind = move(own, down)
        far_left = move(ahead[:, :half], up)
        far_right = move(behind[:, half:], down)
        far = jnp.concatenate([far_left, far_right], axis=1)
        out += [own, behind, far, ahead]
    return jnp.concatenate(out, axis=0)


def local(ainv_anc, l_panel, diag_inv, struct_mask, pieces, tile_owner):
    row_devices = lax.axis_size("row")
    col_devices = lax.axis_size("col")
    row = lax.axis_index("row")
    col = lax.axis_index("col")
    z, k = row // 2, row % 2
    y, x = col // 4, col % 4
    slab_rows, local_rows = l_panel.shape
    block_count = local_rows // AB
    half = local_rows // 2
    supernode = col * slab_rows // W

    keep_blocks = lax.dynamic_slice(struct_mask, (supernode, row * block_count), (1, block_count))
    keep = jnp.broadcast_to(keep_blocks[:, :, None], (1, block_count, AB)).reshape(1, -1) > 0
    lm = jnp.where(keep, l_panel, jnp.zeros_like(l_panel))

    odd = col % 2 == 1
    left, right = lm[:, :half], lm[:, half:]
    own_core, other = [], []
    for p, part in enumerate((jnp.where(odd, right, left), jnp.where(odd, left, right))):
        block = move(part, to_group(p))
        blocks = [block] + [move(block, along("z", s)) for s in (1, 2, 3)]
        own_core.append(jnp.stack(blocks))
        other.append(move(own_core[-1], other_core))

    lm_rows = gathered_rows(lm)

    moving = pack(tile_owner[:, 0], pieces, row_devices * col_devices)
    arrived = lax.all_to_all(moving, BOTH, split_axis=0, concat_axis=0, tiled=True)
    moved_pieces = arrived.astype(jnp.float32)

    first, second = ainv_anc[:half], ainv_anc[half:]

    def by_x(both):
        mine = k == x // 2
        ahead_mine = k == (x + 1) % 4 // 2
        (own_0, own_1), (other_0, other_1) = both
        return (
            jnp.where(mine, other_0, own_0),
            jnp.where(ahead_mine, own_1, other_1),
            jnp.where(ahead_mine, other_1, own_1),
            jnp.where(mine, own_0, other_0),
        )

    def by_y(value):
        return tuple(at_first(value, (z - y - step) % 4) for step in (2, 1, -1, 0))

    rows_x = by_x((own_core, other))
    rows_y = by_y(jnp.stack(own_core + other, axis=1))
    far_a, far_b = times(rows_x[0], first), times(rows_y[0], second)
    products_a = [far_a] + [times(v, first) for v in rows_x[1:]]
    products_b = [far_b] + [times(v, second) for v in rows_y[1:]]
    sums_a = jnp.concatenate(ring_sum("x", *products_a), axis=-1)
    sums_b = jnp.concatenate(ring_sum("y", *products_b), axis=-1)
    small_a, small_b = sums_a.astype(jnp.bfloat16), sums_b.astype(jnp.bfloat16)
    out_a = direct_sum("y", *by_y(small_a)[:3], by_y(sums_a)[3])
    pairs = lambda v: ((v[0], v[1]), (v[2], v[3]))
    out_b = direct_sum("x", *by_x(pairs(small_b))[:3], by_x(pairs(sums_b))[3])
    product = jnp.concatenate([out_a, out_b], axis=-1)
    upper = jnp.where(keep, -product, jnp.zeros_like(product)).astype(jnp.bfloat16)

    diag_part = lax.dot_general(
        upper, lm_rows, (((1,), (1,)), ((), ())), preferred_element_type=jnp.float32
    ).astype(jnp.bfloat16)
    parts = jnp.moveaxis(diag_part.reshape(slab_rows, row_devices, slab_rows), 1, 0)
    near, paired = rolled(parts[:4], x), rolled(parts[4:], x)
    upper_half = y % 2 == 1
    parts = jnp.concatenate(
        [jnp.where(upper_half, paired, near), jnp.where(upper_half, near, paired)]
    )
    diag_sum = f32(lax.all_to_all(parts, "row", split_axis=0, concat_axis=0, tiled=True)).sum(axis=0)
    return upper, diag_inv - diag_sum, moved_pieces


def solution(mesh):
    in_specs = (
        P("row", "col"),
        P("col", "row"),
        P("col", "row"),
        P(),
        P(BOTH, None, None),
        P(BOTH, None),
    )
    out_specs = (P("col", "row"), P("col", "row"), P(BOTH, None, None))
    return jax.shard_map(local, mesh=mesh, in_specs=in_specs, out_specs=out_specs, check_vma=False)
```
